512 devices in a mesh: ctx: 64 (over z, y), tp: 8 (over x, core).
Axes of the slice: x: 4, y: 4, z: 16, core: 2. Of those that a mesh axis runs over, the one named last changes fastest.
Arguments:
- rotated_asking_vectors: bfloat16 [2, 2048, 64, 128], P(None, ('ctx', 'tp')), may hold values from -6 to 6
- rotated_match_vectors: bfloat16 [2, 2048, 8, 128], P(None, ('ctx', 'tp')), may hold values from -6 to 6
- content_vectors: bfloat16 [2, 2048, 8, 128], P(None, ('ctx', 'tp')), may hold values from -6 to 6
- result_cotangent: bfloat16 [2, 2048, 64, 128], P(None, ('ctx', 'tp')), may hold values from -6 to 6
Outputs:
- attended: bfloat16 [2, 2048, 64, 128], P(None, ('ctx', 'tp'))
- grad_query: bfloat16 [2, 2048, 64, 128], P(None, ('ctx', 'tp'))
- grad_key: bfloat16 [2, 2048, 8, 128], P(None, ('ctx', 'tp'))
- grad_value: bfloat16 [2, 2048, 8, 128], P(None, ('ctx', 'tp'))
The draws below stay inside these ranges and needn't reach their ends.
All inputs are finite; a program needn't handle non-finite values.
Results may differ from the reference program's by a relative error of at most 0.002.
Values may be sent and summed in bfloat16 or wider, within the bound.
A program may use at most 64 MiB of HBM per device.

```python
import jax
import jax.numpy as jnp
from jax import lax

ASKING_HEAD_COUNT = 64
SHARED_HEAD_COUNT = 8
HEAD_WIDTH = 128
DEPTH_COUNT = 2
WINDOW_LENGTH = 2048
QUERIES_PER_SHARED = 8


def level_of(key, extent, cuts, least, top_value):
    loudness, own = 1.0, jax.random.fold_in(key, 6)
    for position, parts in cuts:
        steps = jnp.exp(jax.random.uniform(jax.random.fold_in(own, position), (parts,), jnp.float32, least / len(cuts), top_value / len(cuts)))
        loudness = loudness * jnp.repeat(steps, extent[position] // parts).reshape([-1 if axis == position else 1 for axis in range(len(extent))])
    return loudness


def noise(rng, shape, spread, reach, pieces=(), kind=jnp.bfloat16):
    result = spread * jax.random.normal(rng, shape, jnp.float32)
    if pieces:
        result = result * level_of(rng, shape, pieces, -0.22, 0.18)
    return jnp.clip(result, -reach, reach).astype(kind)


def setup_inputs(seed: int = 0) -> dict:
    key_list = jax.random.split(jax.random.key(seed), 5)
    return {
        "rotated_asking_vectors": noise(key_list[0], (DEPTH_COUNT, WINDOW_LENGTH, ASKING_HEAD_COUNT, HEAD_WIDTH), 1.0, 6.0, ((1, 512),)),
        "rotated_match_vectors": noise(key_list[1], (DEPTH_COUNT, WINDOW_LENGTH, SHARED_HEAD_COUNT, HEAD_WIDTH), 1.0, 6.0, ((1, 512),)),
        "content_vectors": noise(key_list[2], (DEPTH_COUNT, WINDOW_LENGTH, SHARED_HEAD_COUNT, HEAD_WIDTH), 1.0, 6.0, ((1, 512),)),
        "result_cotangent": noise(key_list[3], (DEPTH_COUNT, WINDOW_LENGTH, ASKING_HEAD_COUNT, HEAD_WIDTH), 1.0, 6.0, ((1, 512),)),
    }


def head_group(operands):
    query_group, key_group, value_group, grad_group = operands
    softmax_scale = HEAD_WIDTH ** -0.5
    places = jnp.arange(WINDOW_LENGTH, dtype=jnp.int32)
    causal_mask = places[None, :] <= places[:, None]
    scores = jnp.einsum("gid,jd->gij", query_group, key_group, precision=lax.Precision.HIGHEST) * softmax_scale
    scores = jnp.where(causal_mask[None], scores, -jnp.inf)
    highest = jnp.max(scores, axis=-1, keepdims=True)
    log_norm = highest + jnp.log(jnp.sum(jnp.exp(scores - highest), axis=-1, keepdims=True))
    probabilities = jnp.exp(scores - log_norm)
    attended = jnp.einsum("gij,jd->gid", probabilities, value_group, precision=lax.Precision.HIGHEST).astype(jnp.bfloat16)
    saved_out = lax.optimization_barrier(attended).astype(jnp.float32)
    row_delta = jnp.sum(grad_group * saved_out, axis=-1, keepdims=True)
    prob_grad = jnp.einsum("gid,jd->gij", grad_group, value_group, precision=lax.Precision.HIGHEST)
    dscore = probabilities * (prob_grad - row_delta)
    query_grad = softmax_scale * jnp.einsum("gij,jd->gid", dscore, key_group, precision=lax.Precision.HIGHEST)
    key_grad = softmax_scale * jnp.einsum("gij,gid->jd", dscore, query_group, precision=lax.Precision.HIGHEST)
    value_grad = jnp.einsum("gij,gid->jd", probabilities, grad_group, precision=lax.Precision.HIGHEST)
    return attended, query_grad.astype(jnp.bfloat16), key_grad.astype(jnp.bfloat16), value_grad.astype(jnp.bfloat16)


def reference(rotated_asking_vectors, rotated_match_vectors, content_vectors, result_cotangent):
    outputs = ([], [], [], [])
    for depth_position in range(DEPTH_COUNT):
        expanded_asking_vectors = rotated_asking_vectors[depth_position].astype(jnp.float32).reshape(WINDOW_LENGTH, SHARED_HEAD_COUNT, QUERIES_PER_SHARED, HEAD_WIDTH).transpose(1, 2, 0, 3)
        expanded_cotangent = result_cotangent[depth_position].astype(jnp.float32).reshape(WINDOW_LENGTH, SHARED_HEAD_COUNT, QUERIES_PER_SHARED, HEAD_WIDTH).transpose(1, 2, 0, 3)
        key_wide = rotated_match_vectors[depth_position].astype(jnp.float32).transpose(1, 0, 2)
        value_wide = content_vectors[depth_position].astype(jnp.float32).transpose(1, 0, 2)
        attended, query_grad, key_grad, value_grad = lax.map(head_group, (expanded_asking_vectors, key_wide, value_wide, expanded_cotangent))
        outputs[0].append(attended.transpose(2, 0, 1, 3).reshape(WINDOW_LENGTH, ASKING_HEAD_COUNT, HEAD_WIDTH))
        outputs[1].append(query_grad.transpose(2, 0, 1, 3).reshape(WINDOW_LENGTH, ASKING_HEAD_COUNT, HEAD_WIDTH))
        outputs[2].append(key_grad.transpose(1, 0, 2))
        outputs[3].append(value_grad.transpose(1, 0, 2))
    return (jnp.stack(outputs[0]), jnp.stack(outputs[1]), jnp.stack(outputs[2]), jnp.stack(outputs[3]))
```

```python
from functools import partial

import jax
import jax.numpy as jnp
from jax import lax
from jax.experimental import pallas as pl
from jax.experimental.pallas import tpu as pltpu
from jax.sharding import PartitionSpec as P

MESH = pl.DeviceIdType.MESH
F32, BF16 = jnp.float32, jnp.bfloat16
masked_score = -1e30
NX, CORES = 4, 2
REACH = 1


def dot(a, b):
    return lax.dot_general(a, b, (((1,), (0,)), ((), ())), preferred_element_type=F32)


def kernel(
    sizes,
    q_ref,
    k_ref,
    v_ref,
    g_ref,
    att_ref,
    dq_ref,
    gk_ref,
    gv_ref,
    narrow,
    kvp,
    kvin,
    qin,
    kv,
    qs,
    gs,
    qt,
    gt,
    top,
    sc,
    dp,
    pb,
    db,
    kt2,
    vt2,
    att_t,
    dq_t,
    acc,
    pin,
    recv,
    oq,
    okv,
    okv_in,
    kv_s,
    kv_r,
    q_s,
    q_r,
    g_s,
    g_r,
    h_s,
    h_r,
    p_s,
    p_r,
    r_s,
    r_r,
    o_s,
    o_r,
    f_s,
    f_r,
    local,
):
    layers, G, nx, ny, NZ, t, heads, width = sizes
    PN = nx * ny
    H = NZ // 2
    R = REACH
    HK = PN * t
    BK = 2 * HK
    rows = PN * t * heads
    scale = width**-0.5
    ctx, tp = lax.axis_index("ctx"), lax.axis_index("tp")
    z, y = ctx // ny, ctx % ny
    x, c = tp // CORES, tp % CORES
    me = y * nx + x

    def at(p, core):
        return {"ctx": z * ny + p // nx, "tp": (p % nx) * CORES + core}

    def up(i):
        return {"ctx": lax.rem(z + i, NZ) * ny + y, "tp": tp}

    def down(i):
        return {"ctx": lax.rem(z + NZ - i, NZ) * ny + y, "tp": tp}

    partner = {"ctx": ctx, "tp": x * CORES + 1 - c}

    def remote(src, dst, s, r, to):
        return pltpu.make_async_remote_copy(src, dst, s, r, to, MESH)

    def group(ref, p):
        return ref.at[p // G, :, pl.ds(pl.multiple_of((p % G) * heads, heads), heads), :]

    def kv_copy(to, core, src_core, src):
        return remote(kvp.at[to], kvin.at[src_core, src], kv_s.at[core, to], kv_r.at[src_core, src], at(to, core))

    def q_copy(kind, to, src):
        return remote(
            group((q_ref, g_ref)[kind], to), qin.at[kind, src], q_s.at[kind, to], q_r.at[kind, src], at(to, c)
        )

    def g_copy(plus, i, b):
        return remote(
            kv.at[b, c], kv.at[b, c], g_s.at[plus, i - 1, b], g_r.at[b], up(i) if plus else down(i)
        )

    def h_copy(b, half):
        return remote(kv.at[b, half], kv.at[b, half], h_s.at[b], h_r.at[b], partner)

    def p_copy(b):
        return remote(acc.at[b, 1 - c], pin.at[b], p_s.at[b], p_r.at[b], partner)

    def r_copy(plus, i, b):
        return remote(
            acc.at[b, c],
            recv.at[plus, i - 1, b],
            r_s.at[b],
            r_r.at[plus, i - 1, b],
            up(i) if plus else down(i),
        )

    def o_copy(kind, to, src):
        return remote(
            oq.at[kind, to], group((att_ref, dq_ref)[kind], src), o_s.at[kind, to], o_r.at[kind, src], at(to, c)
        )

    def f_copy(to, src):
        return remote(okv.at[to], okv_in.at[src], f_s.at[to], f_r.at[src], at(to, c))

    def each_peer(fn):
        @pl.loop(1, PN)
        def _(d):
            fn(lax.rem(me + d, PN))

    def active(b, s):
        return (s > b) | (lax.rem(s, R) == 0)

    barrier = pltpu.get_barrier_semaphore()

    def greet(p):
        for core in range(CORES):
            pl.semaphore_signal(barrier, 1, device_id=at(p, core), device_id_type=MESH)

    pl.semaphore_signal(barrier, 1, device_id=partner, device_id_type=MESH)
    for i in range(1, R + 1):
        pl.semaphore_signal(barrier, 1, device_id=up(i), device_id_type=MESH)
        pl.semaphore_signal(barrier, 1, device_id=down(i), device_id_type=MESH)
    each_peer(greet)

    for l in range(layers):
        narrow[l, 0 : t * G] = k_ref[l].astype(F32).reshape(t * G, width)
        narrow[l, t * G : 2 * t * G] = v_ref[l].astype(F32).reshape(t * G, width)
    for l in range(layers):
        for g in range(G):
            kvp[l * G + g] = narrow[l, pl.ds(g, 2 * t, stride=G), :].astype(BF16)

    pl.semaphore_wait(barrier, 2 * (PN - 1) + 1 + 2 * R)

    def send_kv(p):
        for core in range(CORES):
            kv_copy(p, core, c, me).start()

    each_peer(send_kv)
    kv_copy(me, 1 - c, c, me).start()
    own = [pltpu.make_async_copy(kvp.at[me], kvin.at[c, me], local.at[0])]
    for kind, ref in enumerate((q_ref, g_ref)):
        each_peer(lambda p: q_copy(kind, p, me).start())
        own.append(pltpu.make_async_copy(group(ref, me), qin.at[kind, me], local.at[1 + kind]))
    for copy in own:
        copy.start()

    def land_kv(p):
        for core in range(CORES):
            kv_copy(me, c, core, p).wait_recv()

    own[0].wait()
    kv_copy(me, c, 1 - c, me).wait_recv()
    each_peer(land_kv)
    for h in range(CORES):
        part = kvin[h].astype(F32)
        for s in range(PN):
            for kind in range(2):
                narrow[kind, s * t : (s + 1) * t] = part[s, kind * t : (kind + 1) * t]
        for kind in range(2):
            kv[z, h, kind] = narrow[kind, 0:HK].astype(BF16)

    def relay(b, s):
        for i in range(1, R + 1):

            @pl.when((s + i <= H) & (z + i < NZ))
            def _():
                g_copy(1, i, b).start()

    def relay_down(b, s):
        for i in range(1, R + 1):

            @pl.when((s + i < H) & active(b, s + i))
            def _():
                g_copy(0, i, b).start()

    relay(z, 0)

    @pl.when(z <= H - 2)
    def _():
        relay_down(z, 0)

    for kind, (mine, turned) in enumerate(((qs, qt), (gs, gt))):
        own[1 + kind].wait()
        each_peer(lambda p: q_copy(kind, me, p).wait_recv())
        wide = qin[kind].astype(F32).reshape(rows, width)
        mine[...] = wide.astype(BF16)
        turned[...] = wide.T.astype(BF16)

    def block(b, diagonal=False):
        K = kv[b, :, 0].reshape(BK, width)
        V = kv[b, :, 1].reshape(BK, width)
        scores = dot(K, qt[...])
        if diagonal:
            row = lax.broadcasted_iota(jnp.int32, (1, rows), 1)
            key = lax.broadcasted_iota(jnp.int32, (BK, 1), 0)
            row_token = row // (t * heads) * (2 * t) + c * t + row % (t * heads) // heads
            key_token = key % HK // t * (2 * t) + key // HK * t + key % t
            scores = jnp.where(key_token <= row_token, scores, masked_score)
            top[...] = jnp.max(scores, axis=0, keepdims=True)
        else:
            top[...] = jnp.maximum(top[...], jnp.max(scores, axis=0, keepdims=True))
        sc[b] = scores
        dp[b] = dot(V, gt[...])
        for ref, value in ((kt2, K), (vt2, V)):
            turned = value.astype(F32).T.astype(BF16)
            ref[b, :, 0:BK] = turned
            ref[b, :, BK : 2 * BK] = turned

    block(z, True)

    def lower(s):
        return z - s

    def wrapped(s):
        return lax.rem(z + s, NZ)

    def compute(s):
        b = lower(s)

        @pl.when(b >= 0)
        def _():
            h_copy(b, 1 - c).wait_recv()
            block(b)

        b2 = wrapped(s)

        @pl.when((s < H) & (b2 < z))
        def _():
            h_copy(b2, 1 - c).wait_recv()
            block(b2)

    @pl.loop(1, H + 1)
    def _(s):
        b = lower(s)

        @pl.when(b >= 0)
        def _():
            g_copy(1, 1, b).wait_recv()

            @pl.when(lax.rem(s, R) == 0)
            def _():
                relay(b, s)

            h_copy(b, c).start()

        b2 = wrapped(s)

        @pl.when((s < H) & (b2 <= H - 2) & active(b2, s))
        def _():
            g_copy(0, 1, b2).wait_recv()

            @pl.when(lax.rem(s, R) == 0)
            def _():
                relay_down(b2, s)

            @pl.when(b2 < z)
            def _():
                h_copy(b2, c).start()

        @pl.when(s > 1)
        def _():
            compute(s - 1)

    compute(H)

    highest = top[...]
    top[...] = jnp.zeros_like(top)

    @pl.loop(0, z + 1)
    def _(b):
        e = jnp.exp((sc[b] - highest) * scale)
        sc[b] = e
        top[...] += jnp.sum(e, axis=0, keepdims=True)

    inverse = 1.0 / top[...]
    att_t[...] = jnp.zeros_like(att_t)

    @pl.loop(0, z + 1)
    def _(b):
        prob = sc[b] * inverse
        sc[b] = prob
        high = prob.astype(BF16)
        pb[b, 0:BK] = high
        pb[b, BK : 2 * BK] = (prob - high.astype(F32)).astype(BF16)
        att_t[...] += dot(vt2[b], pb[b])

    rounded = att_t[...].astype(BF16).astype(F32)
    delta = jnp.sum(rounded * gt[...].astype(F32), axis=0, keepdims=True)
    oq[0] = rounded.T.astype(BF16).reshape(PN, t, heads, width)
    each_peer(lambda p: o_copy(0, p, me).start())
    o_own = [
        pltpu.make_async_copy(oq.at[kind, me], group((att_ref, dq_ref)[kind], me), local.at[3 + kind])
        for kind in range(2)
    ]
    o_own[0].start()
    dq_t[...] = jnp.zeros_like(dq_t)

    def back(b):
        ds = sc[b] * (dp[b] - delta)
        high = ds.astype(BF16)
        db[0:BK] = high
        db[BK : 2 * BK] = (ds - high.astype(F32)).astype(BF16)
        both = db[...]
        dq_t[...] += dot(kt2[b], both)
        dk = dot(both, qs[...])
        dv = dot(pb[b], gs[...])
        for kind, value in enumerate((dk, dv)):
            value = value[0:BK] + value[BK : 2 * BK]
            for h in range(CORES):
                acc[b, h, kind] = value[h * HK : (h + 1) * HK]
        p_copy(b).start()

    def stage(s):
        b = lower(s)

        @pl.when(b >= 0)
        def _():
            back(b)

        b2 = wrapped(s)

        @pl.when((s < H) & (b2 < z))
        def _():
            back(b2)

    def children(b, s):
        for i in range(1, R + 1):

            @pl.when((s + i <= H) & (z + i < NZ))
            def _():
                r_copy(0, i, b).wait_recv()
                acc[b, c] += recv[0, i - 1, b]

    def children_up(b, s):
        for i in range(1, R + 1):

            @pl.when((s + i < H) & active(b, s + i))
            def _():
                r_copy(1, i, b).wait_recv()
                acc[b, c] += recv[1, i - 1, b]

    def mine(b):
        p_copy(b).wait_recv()
        acc[b, c] += pin[b]

    def fold(s):
        b = lower(s)

        @pl.when(b >= 0)
        def _():
            mine(b)

            @pl.when(lax.rem(s, R) == 0)
            def _():
                children(b, s)

            for i in range(1, R + 1):

                @pl.when(lax.rem(s - 1, R) + 1 == i)
                def _():
                    r_copy(0, i, b).start()

        b2 = wrapped(s)

        @pl.when((s < H) & (b2 <= H - 2) & active(b2, s))
        def _():
            @pl.when(b2 < z)
            def _():
                mine(b2)

            @pl.when(b2 > z)
            def _():
                acc[b2, c] = jnp.zeros(acc.shape[2:], F32)

            @pl.when(lax.rem(s, R) == 0)
            def _():
                children_up(b2, s)

            for i in range(1, R + 1):

                @pl.when(lax.rem(s - 1, R) + 1 == i)
                def _():
                    r_copy(1, i, b2).start()

    stage(H)

    @pl.loop(0, H - 1)
    def _(j):
        stage(H - 1 - j)
        fold(H - j)

    back(z)
    oq[1] = (dq_t[...] * scale).T.astype(BF16).reshape(PN, t, heads, width)
    each_peer(lambda p: o_copy(1, p, me).start())
    o_own[1].start()
    fold(1)
    mine(z)
    children(z, 0)

    @pl.when(z <= H - 2)
    def _():
        children_up(z, 0)

    total = (acc[z, c, 0] * scale, acc[z, c, 1])
    for kind in range(2):
        for s in range(PN):
            okv_wide = total[kind][s * t : (s + 1) * t]
            narrow[kind * 0 + 0, s * 2 * t + kind * t : s * 2 * t + (kind + 1) * t] = okv_wide
    okv[...] = narrow[0, 0 : PN * 2 * t].reshape(PN, 2 * t, width).astype(BF16)
    each_peer(lambda p: f_copy(p, me).start())
    f_own = pltpu.make_async_copy(okv.at[me], okv_in.at[me], local.at[5])
    f_own.start()

    f_own.wait()
    each_peer(lambda p: f_copy(me, p).wait_recv())
    for l in range(layers):
        narrow[l, 0 : G * 2 * t] = okv_in[l * G : (l + 1) * G].astype(F32).reshape(G * 2 * t, width)
    for l in range(layers):
        for i in range(t):
            gk_ref[l, i] = narrow[l, pl.ds(i, G, stride=2 * t), :].astype(BF16)
            gv_ref[l, i] = narrow[l, pl.ds(t + i, G, stride=2 * t), :].astype(BF16)

    for kind in range(2):
        o_own[kind].wait()

    def finish(p):
        for core in range(CORES):
            kv_copy(p, core, c, me).wait_send()
        for kind in range(2):
            q_copy(kind, p, me).wait_send()
            o_copy(kind, p, me).wait_send()
            o_copy(kind, me, p).wait_recv()
        f_copy(p, me).wait_send()

    each_peer(finish)
    kv_copy(me, 1 - c, c, me).wait_send()
    p_copy(z).wait_send()

    def relayed(b, s):
        for i in range(1, R + 1):

            @pl.when((s + i <= H) & (z + i < NZ))
            def _():
                g_copy(1, i, b).wait_send()

    def relayed_down(b, s):
        for i in range(1, R + 1):

            @pl.when((s + i < H) & active(b, s + i))
            def _():
                g_copy(0, i, b).wait_send()

    relayed(z, 0)

    @pl.when(z <= H - 2)
    def _():
        relayed_down(z, 0)

    @pl.loop(1, H + 1)
    def _(s):
        b = lower(s)

        @pl.when(b >= 0)
        def _():
            h_copy(b, c).wait_send()
            p_copy(b).wait_send()
            r_copy(0, 1, b).wait_send()

            @pl.when(lax.rem(s, R) == 0)
            def _():
                relayed(b, s)

        b2 = wrapped(s)

        @pl.when((s < H) & (b2 <= H - 2) & active(b2, s))
        def _():
            r_copy(1, 1, b2).wait_send()

            @pl.when(b2 < z)
            def _():
                h_copy(b2, c).wait_send()
                p_copy(b2).wait_send()

            @pl.when(lax.rem(s, R) == 0)
            def _():
                relayed_down(b2, s)


def on_device(q, k, v, g):
    layers, t, head_count, width = q.shape
    G = k.shape[2]
    heads = head_count // G
    ctx_n, tp_n = lax.axis_size("ctx"), lax.axis_size("tp")
    nx = tp_n // CORES
    ny = layers * G // nx
    NZ = ctx_n // ny
    PN = nx * ny
    HK = PN * t
    BK = 2 * HK
    rows = PN * t * heads

    vmem = pl.BlockSpec(memory_space=pltpu.VMEM)
    sem = pltpu.SemaphoreType.DMA
    V = pltpu.VMEM
    whole_shape = jax.ShapeDtypeStruct(q.shape, BF16)
    kv_shape = jax.ShapeDtypeStruct(k.shape, BF16)
    deep = max(HK * 2, 2 * t * G)
    return pl.pallas_call(
        partial(kernel, (layers, G, nx, ny, NZ, t, heads, width)),
        out_shape=(whole_shape, whole_shape, kv_shape, kv_shape),
        in_specs=[vmem] * 4,
        out_specs=(vmem,) * 4,
        scratch_shapes=[
            V((2, deep, width), F32),
            V((PN, 2 * t, width), BF16),
            V((CORES, PN, 2 * t, width), BF16),
            V((2, PN, t, heads, width), BF16),
            V((NZ, CORES, 2, HK, width), BF16),
            V((rows, width), BF16),
            V((rows, width), BF16),
            V((width, rows), BF16),
            V((width, rows), BF16),
            V((1, rows), F32),
            V((NZ, BK, rows), F32),
            V((NZ, BK, rows), F32),
            V((NZ, 2 * BK, rows), BF16),
            V((2 * BK, rows), BF16),
            V((NZ, width, 2 * BK), BF16),
            V((NZ, width, 2 * BK), BF16),
            V((width, rows), F32),
            V((width, rows), F32),
            V((NZ, CORES, 2, HK, width), F32),
            V((NZ, 2, HK, width), F32),
            V((2, REACH, NZ, 2, HK, width), F32),
            V((2, PN, t, heads, width), BF16),
            V((PN, 2 * t, width), BF16),
            V((PN, 2 * t, width), BF16),
            sem((CORES, PN)),
            sem((CORES, PN)),
            sem((2, PN)),
            sem((2, PN)),
            sem((2, REACH, NZ)),
            sem((NZ,)),
            sem((NZ,)),
            sem((NZ,)),
            sem((NZ,)),
            sem((NZ,)),
            sem((NZ,)),
            sem((2, REACH, NZ)),
            sem((2, PN)),
            sem((2, PN)),
            sem((PN,)),
            sem((PN,)),
            sem((6,)),
        ],
        compiler_params=pltpu.CompilerParams(collective_id=0, has_side_effects=True),
    )(q, k, v, g)


def solution(mesh):
    spec = P(None, ("ctx", "tp"), None, None)
    return jax.shard_map(
        on_device, mesh=mesh, in_specs=(spec,) * 4, out_specs=(spec,) * 4, check_vma=False
    )
```
